32 devices in a mesh: groups: 2 (over y), plane: 4 (over z), depth: 2 (over x), tok: 2 (over core).
Axes of the slice: x: 2, y: 2, z: 4, core: 2. Of those that a mesh axis runs over, the one named last changes fastest.
Arguments:
- tokens: bfloat16 [256, 2048], P(('groups', 'plane', 'depth', 'tok')), parts along dimension 0, may hold values from -6 to 6
- expert_ids: int32 [256, 4], P(('groups', 'plane', 'depth', 'tok')), parts along dimension 0, may hold values from 0 to 3, as said below
- slot_index: int32 [256, 4], P(('groups', 'plane', 'depth', 'tok')), parts along dimension 0, may hold values from 0 to 7, as said below
- route_weight: bfloat16 [256, 4], P(('groups', 'plane', 'depth', 'tok')), parts along dimension 0, may hold values from 0.099609375 to 1
- shared_gate: bfloat16 [2048], replicated, may hold values from -0.125 to 0.125
- shared_gate_up: bfloat16 [2, 2048, 5632], P(None, None, 'plane'), may hold values from -0.125 to 0.125
- shared_down: bfloat16 [5632, 2048], P('plane'), may hold values from -0.078125 to 0.078125
- expert_gate_up: bfloat16 [4, 2, 2048, 1408], P('plane', None, None, ('depth', 'tok')), may hold values from -0.125 to 0.125
- expert_down: bfloat16 [4, 1408, 2048], P('plane', ('depth', 'tok')), may hold values from -0.15625 to 0.15625
Outputs:
- mixed: bfloat16 [256, 2048], P(('groups', 'plane', 'depth', 'tok')), parts along dimension 0
The draws below stay inside these ranges and needn't reach their ends.
There are 2 independent parts, one for each index of `groups`. The reference program is written for one: setup_inputs(seed, part) draws one part's arguments, and reference() takes and returns one part's arrays. A program takes and returns all parts, laid end to end along the dimension named above; an argument that names none is the same for every part. Nothing has to cross between parts.
Inputs may be any that keep to these rules, and one draw needn't show every extreme that they name: `expert_ids`: each row names 4 different experts. Among the choices of the rows of one device that name the same expert, slot_index takes each value from 0 to their count minus one exactly once, in an order that varies from draw to draw; the capacity 8 is filled on some devices.
All inputs are finite; a program needn't handle non-finite values.
Results may differ from the reference program's by a relative error of at most 0.019.
Values may be sent and summed in bfloat16 or wider, within the bound.
A program may use at most 64 MiB of HBM per device.

```python
import math
import jax
import jax.numpy as jnp
from jax import lax

D = 2048
FF_SH = 5632
FF_EX = 1408
TOP = 4
TOK_DEV = 8
TOKENS = 128
EXPERTS = 4
SHARDS = 4
CAP = 8


def route_table(key):
    base_key = jax.random.fold_in(key, 11)
    first_key, second_key = jax.random.split(base_key)
    order_key = jax.random.fold_in(base_key, 29)
    ranking = jax.random.permutation(first_key, EXPERTS)
    favour = jnp.where(ranking < 4, 256, 0).astype(jnp.int32)
    noise = jax.random.randint(second_key, (TOKENS, EXPERTS), 0, 1024, dtype=jnp.int32)
    scores = (noise + favour[None, :]) * EXPERTS + jnp.arange(EXPERTS, dtype=jnp.int32)[None, :]
    best_values, chosen = lax.top_k(scores, TOP)
    chosen = chosen.astype(jnp.int32)
    entries = TOK_DEV * TOP
    grouped = chosen.reshape(TOKENS // TOK_DEV, entries)
    priority = jax.random.randint(order_key, (TOKENS // TOK_DEV, entries), 0, 1 << 20, dtype=jnp.int32)
    priority = priority * entries + jnp.arange(entries, dtype=jnp.int32)[None, :]
    before = (priority[:, None, :] < priority[:, :, None]).astype(jnp.int32)
    same = (grouped[:, None, :] == grouped[:, :, None]).astype(jnp.int32)
    slots = jnp.sum(before * same, axis=2).reshape(TOKENS, TOP)
    return (chosen, slots.astype(jnp.int32))


def draw_expert_ids(key, part):
    return route_table(key)[0]


def draw_slot_index(key, part):
    return route_table(key)[1]


def block_levels(rng, dims, cuts, smallest, largest):
    factor_of, own = 1.0, jax.random.fold_in(rng, 6)
    for dim, blocks in cuts:
        steps = jnp.exp(jax.random.uniform(jax.random.fold_in(own, dim), (blocks,), jnp.float32, smallest / len(cuts), largest / len(cuts)))
        factor_of = factor_of * jnp.repeat(steps, dims[dim] // blocks).reshape([-1 if axis == dim else 1 for axis in range(len(dims))])
    return factor_of


def gaussian(key, dims, deviation, limit, pieces=(), kind=jnp.bfloat16):
    drawn = deviation * jax.random.normal(key, dims, jnp.float32)
    if pieces:
        drawn = drawn * block_levels(key, dims, pieces, -0.22, 0.18)
    return jnp.clip(drawn, -limit, limit).astype(kind)


def setup_inputs(seed: int = 0, part: int = 0) -> dict:
    key_of = jax.random.split(jax.random.key(seed), 10)
    part_splits = jax.random.split(jax.random.fold_in(key_of[9], part), 10)
    tokens = gaussian(part_splits[0], (TOKENS, D), 1.0, 6.0, ((0, 16),))
    expert_ids = draw_expert_ids(jax.random.fold_in(jax.random.fold_in(key_of[9], part), 71), part)
    slot_index = draw_slot_index(jax.random.fold_in(jax.random.fold_in(key_of[9], part), 71), part)
    route_weight = jnp.clip(jnp.exp(math.log(1.0) - 2.306499 * jax.random.uniform(part_splits[3], (TOKENS, TOP), jnp.float32) ** block_levels(part_splits[3], (TOKENS, TOP), ((0, 16),), -0.2, 0.2)), 0.099609375, 1.0).astype(jnp.bfloat16)
    shared_gate = gaussian(key_of[4], (D,), D ** -0.5, 0.125)
    shared_gate_up = gaussian(key_of[5], (2, D, FF_SH), D ** -0.5, 0.125, ((2, 4),))
    shared_down = gaussian(key_of[6], (FF_SH, D), FF_SH ** -0.5, 0.078125, ((0, 4),))
    expert_gate_up = gaussian(key_of[7], (EXPERTS, 2, D, FF_EX), D ** -0.5, 0.125, ((0, 4), (3, 4)))
    expert_down = gaussian(key_of[8], (EXPERTS, FF_EX, D), FF_EX ** -0.5, 0.15625, ((0, 4), (1, 4)))
    return {"tokens": tokens, "expert_ids": expert_ids, "slot_index": slot_index, "route_weight": route_weight, "shared_gate": shared_gate, "shared_gate_up": shared_gate_up, "shared_down": shared_down, "expert_gate_up": expert_gate_up, "expert_down": expert_down}


def reference(tokens, expert_ids, slot_index, route_weight, shared_gate, shared_gate_up, shared_down, expert_gate_up, expert_down):
    gate_proj = jnp.dot(tokens, shared_gate_up[0], preferred_element_type=jnp.float32)
    up_proj = jnp.dot(tokens, shared_gate_up[1], preferred_element_type=jnp.float32)
    shared_hidden = (jax.nn.silu(gate_proj) * up_proj).astype(jnp.bfloat16)
    shared_out = jnp.dot(shared_hidden, shared_down, preferred_element_type=jnp.float32)
    shared_scale = jax.nn.sigmoid(jnp.dot(tokens, shared_gate, preferred_element_type=jnp.float32))
    blocks = TOKENS // TOK_DEV
    rows_each = blocks * CAP
    token_index = jnp.arange(TOKENS, dtype=jnp.int32)[:, None] + jnp.zeros((1, TOP), jnp.int32)
    kept_mask = slot_index < CAP
    position = expert_ids * rows_each + (token_index // TOK_DEV) * CAP + slot_index
    position = jnp.where(kept_mask, position, EXPERTS * rows_each).reshape(-1)
    source = jnp.zeros((EXPERTS * rows_each,), jnp.int32).at[position].set(token_index.reshape(-1), mode="drop")
    factor = jnp.zeros((EXPERTS * rows_each,), jnp.float32).at[position].set(route_weight.reshape(-1).astype(jnp.float32), mode="drop")
    source = source.reshape(EXPERTS, rows_each)
    factor = factor.reshape(EXPERTS, rows_each)
    block_width = FF_EX // SHARDS

    def one_expert(inputs):
        picked, factor_row, weights_gate_up, weights_down = inputs
        token_rows = tokens[picked]
        gate_part = jnp.dot(token_rows, weights_gate_up[0], preferred_element_type=jnp.float32)
        up_part = jnp.dot(token_rows, weights_gate_up[1], preferred_element_type=jnp.float32)
        hidden = (jax.nn.silu(gate_part) * up_part).astype(jnp.bfloat16)
        partials = jnp.einsum("rsf,sfd->rsd", hidden.reshape(-1, SHARDS, block_width).astype(jnp.float32),
                              weights_down.reshape(SHARDS, block_width, D).astype(jnp.float32),
                              precision=lax.Precision.HIGHEST)
        rounded = lax.optimization_barrier(partials.astype(jnp.bfloat16))
        summed = jnp.sum(rounded.astype(jnp.float32), axis=1)
        return summed * factor_row[:, None]

    contrib = lax.map(one_expert, (source, factor, expert_gate_up, expert_down))
    routed = jnp.zeros((TOKENS, D), jnp.float32).at[source.reshape(-1)].add(contrib.reshape(-1, D))
    return (shared_scale[:, None] * shared_out + routed).astype(jnp.bfloat16)
```

```python
import functools

import jax
import jax.numpy as jnp
from jax import lax
from jax.experimental import pallas as pl
from jax.experimental.pallas import tpu as pltpu
from jax.sharding import PartitionSpec as P


def gated_rows(token_rows, gate_up):
    gate_part = jnp.dot(token_rows, gate_up[0], preferred_element_type=jnp.float32)
    up_part = jnp.dot(token_rows, gate_up[1], preferred_element_type=jnp.float32)
    return (jax.nn.silu(gate_part) * up_part).astype(jnp.bfloat16)


def expert_rows(received, gate_up, down_proj):
    hidden = gated_rows(lax.all_gather(received, ("depth", "tok"), axis=0, tiled=True), gate_up)
    return lax.psum_scatter(
        jnp.dot(hidden, down_proj, preferred_element_type=jnp.float32).astype(jnp.bfloat16),
        ("depth", "tok"),
        scatter_dimension=0,
        tiled=True,
    ).astype(jnp.float32)


def on_device(
    tokens,
    expert_ids,
    slot_index,
    route_weight,
    shared_gate,
    shared_gate_up,
    shared_down,
    expert_gate_up,
    expert_down,
):
    planes = lax.axis_size("plane")
    tok_rows = tokens.shape[0]
    choose_count = expert_ids.shape[1]
    model_width = tokens.shape[1]
    capacity = max(2, tok_rows * choose_count // planes)
    slot_total = planes * capacity
    local_gate_up = expert_gate_up[0]
    local_down = expert_down[0]
    column = lax.broadcasted_iota(jnp.int32, (slot_total, 1, 1), 0)
    kept_mask = slot_index < capacity
    target = jnp.where(kept_mask, expert_ids * capacity + slot_index, -1)
    matches = target[None, :, :] == column
    spread = jnp.any(matches, axis=2).astype(jnp.bfloat16)
    outgoing = jnp.dot(spread, tokens, preferred_element_type=jnp.float32).astype(jnp.bfloat16)
    outgoing = outgoing.reshape(planes, capacity, model_width)
    routed_slots = lax.all_to_all(
        expert_rows(
            lax.all_to_all(outgoing, "plane", split_axis=0, concat_axis=0, tiled=True),
            local_gate_up,
            local_down,
        ).astype(jnp.bfloat16),
        "plane",
        split_axis=0,
        concat_axis=0,
        tiled=True,
    ).astype(jnp.float32)
    weights = route_weight.astype(jnp.float32)
    combine = jnp.sum(jnp.where(matches, weights[None, :, :], 0.0), axis=2).T
    routed = jnp.dot(
        combine,
        routed_slots.reshape(slot_total, model_width),
        precision=lax.Precision.HIGHEST,
        preferred_element_type=jnp.float32,
    )
    shared_hidden = gated_rows(lax.all_gather(tokens, "plane", axis=0, tiled=True), shared_gate_up)
    shared_out = lax.psum_scatter(
        jnp.dot(shared_hidden, shared_down, preferred_element_type=jnp.float32).astype(
            jnp.bfloat16
        ),
        "plane",
        scatter_dimension=0,
        tiled=True,
    ).astype(jnp.float32)
    shared_scale = jax.nn.sigmoid(jnp.dot(tokens, shared_gate, preferred_element_type=jnp.float32))
    result = shared_scale[:, None] * shared_out + routed
    return result.astype(jnp.bfloat16)


LANES = 128
COLUMN_CHUNKS = 4
MESH = pl.DeviceIdType.MESH


def planes_by_distance(me, planes):
    orders = [sorted((q for q in range(planes) if q != p), key=lambda q: abs(q - p)) for p in range(planes)]
    picked = []
    for place in range(planes - 1):
        value = jnp.int32(orders[0][place])
        for p in range(1, planes):
            value = jnp.where(me == p, jnp.int32(orders[p][place]), value)
        picked.append(value)
    return picked


def block_kernel(
    planes,
    tok_hbm,
    ids_hbm,
    slot_hbm,
    rw_hbm,
    sg_ref,
    sgu_hbm,
    sdn_hbm,
    egu_hbm,
    edn_hbm,
    out_ref,
    xb,
    ids_v,
    slot_v,
    rw_v,
    sgu_v,
    sdn_v,
    egu_v,
    edn_v,
    keep,
    st,
    rt,
    sx,
    rx,
    vkeep,
    sz,
    rz,
    local_sem,
    ag_send,
    ag_recv,
    t_send,
    t_recv,
    x_send,
    x_recv,
    z_send,
    z_recv,
):
    p = lax.axis_index("plane")
    d = lax.axis_index("depth")
    t = lax.axis_index("tok")
    rows, width = tok_hbm.shape
    choices = ids_hbm.shape[1]
    shared_units = sdn_hbm.shape[0]
    panel = sdn_v.shape[0]
    chunks = st.shape[0]
    span = width // chunks
    half = st.shape[1]
    quarter = half // 2
    near = planes_by_distance(p, planes)
    to_x = {"depth": 1 - d}
    to_t = {"tok": 1 - t}

    shard = d * 2 + t
    start = pl.multiple_of(jnp.minimum(shard * panel, shared_units - panel), LANES)

    def local(src, dst, index):
        copy = pltpu.make_async_copy(src, dst, local_sem.at[index])
        copy.start()
        return copy

    tok_copy = local(tok_hbm, xb.at[p, :, pl.ds(0, width)], 0)
    small = [
        local(ids_hbm, ids_v, 1),
        local(slot_hbm, slot_v, 2),
        local(rw_hbm, rw_v, 3),
    ]
    barrier = pltpu.get_barrier_semaphore()
    for peer in [{"plane": q} for q in near] + [to_x, to_t]:
        pl.semaphore_signal(barrier, inc=1, device_id=peer, device_id_type=MESH)
    up_copies = [
        local(egu_hbm.at[0], egu_v, 4),
        local(sgu_hbm.at[:, :, pl.ds(start, panel)], sgu_v, 5),
    ]
    down_copies = [
        local(edn_hbm.at[0], edn_v, 6),
        local(sdn_hbm.at[pl.ds(start, panel), :], sdn_v, 7),
    ]

    for copy in small:
        copy.wait()
    lane = lax.broadcasted_iota(jnp.int32, (rows, LANES), 1)
    ids = ids_v[...]
    slots = slot_v[...]
    weights = rw_v[...].astype(jnp.float32)
    capacity = max(2, rows * choices // planes)
    share = jnp.zeros((rows, LANES), jnp.float32)
    for k in range(choices):
        hit = (ids[:, k : k + 1] == lane) & (slots[:, k : k + 1] < capacity)
        share = share + jnp.where(hit, weights[:, k : k + 1], 0.0)
    xb[p, :, width:] = share.astype(jnp.bfloat16)
    tok_copy.wait()
    pl.semaphore_wait(barrier, planes + 1)

    def block(rel_t, rel_d, q):
        return xb.at[(rel_t * 2 + rel_d) * planes + q]

    pending = []

    def remote(src, dst, send_sem, recv_sem, device):
        copy = pltpu.make_async_remote_copy(
            src_ref=src,
            dst_ref=dst,
            send_sem=send_sem,
            recv_sem=recv_sem,
            device_id=device,
            device_id_type=MESH,
        )
        copy.start()
        pending.append(copy)

    def landed(dst, send_sem, recv_sem):
        pltpu.make_async_remote_copy(
            src_ref=dst,
            dst_ref=dst,
            send_sem=send_sem,
            recv_sem=recv_sem,
            device_id=to_t,
            device_id_type=MESH,
        ).wait_recv()

    for q in reversed(near):
        remote(block(0, 0, p), block(0, 0, p), ag_send.at[0, q], ag_recv.at[0, p], {"plane": q})

    def pass_x(q):
        remote(block(0, 0, q), block(0, 1, q), ag_send.at[1, q], ag_recv.at[1, q], to_x)

    def pass_t(rel_d, q):
        remote(block(0, rel_d, q), block(1, rel_d, q), ag_send.at[2 + rel_d, q], ag_recv.at[2 + rel_d, q], to_t)

    def from_z(q):
        landed(block(0, 0, q), ag_send.at[0, q], ag_recv.at[0, q])
        pass_x(q)
        pass_t(0, q)

    def from_x(q):
        landed(block(0, 1, q), ag_send.at[1, q], ag_recv.at[1, q])
        pass_t(1, q)

    pass_x(p)
    pass_t(0, p)
    from_z(near[0])
    from_x(p)
    for place in range(1, planes - 1):
        from_z(near[place])
        from_x(near[place - 1])
    from_x(near[-1])
    for copy in up_copies:
        copy.wait()
    for rel_d in range(2):
        for q in [p] + near:
            landed(block(1, rel_d, q), ag_send.at[2 + rel_d, q], ag_recv.at[2 + rel_d, q])

    total = xb.shape[0] * rows
    x = xb[:, :, :width].reshape(total, width)

    def gated(gate_up):
        gate_part = jnp.dot(x, gate_up[0], preferred_element_type=jnp.float32)
        up_part = jnp.dot(x, gate_up[1], preferred_element_type=jnp.float32)
        return jax.nn.silu(gate_part) * up_part

    expert_hidden = gated(egu_v).astype(jnp.bfloat16)
    shared_hidden = gated(sgu_v)
    unit = start + lax.broadcasted_iota(jnp.int32, shared_hidden.shape, 1)
    shared_hidden = jnp.where(unit >= shard * panel, shared_hidden, 0.0).astype(jnp.bfloat16)
    column = lax.broadcasted_iota(jnp.int32, (total, LANES), 1)
    meta = xb[:, :, width:].reshape(total, LANES).astype(jnp.float32)
    route = jnp.sum(jnp.where(column == p, meta, 0.0), axis=1, keepdims=True)
    gate_rows = jnp.broadcast_to(sg_ref[...].reshape(1, width), (8, width))
    score = lax.dot_general(x, gate_rows, (((1,), (1,)), ((), ())), preferred_element_type=jnp.float32)
    scale = jax.nn.sigmoid(score[:, :1])

    for copy in down_copies:
        copy.wait()
    for c in range(chunks):
        cols = pl.ds(c * span, span)
        part = route * jnp.dot(expert_hidden, edn_v[:, cols], preferred_element_type=jnp.float32)
        part = part + scale * jnp.dot(shared_hidden, sdn_v[:, cols], preferred_element_type=jnp.float32)
        st[c] = part[half:].astype(jnp.bfloat16)
        remote(st.at[c], rt.at[c], t_send.at[c], t_recv.at[c], to_t)
        keep[c] = part[:half]
    for c in range(chunks):
        landed(rt.at[c], t_send.at[c], t_recv.at[c])
        sx[c] = (keep[c, quarter:] + rt[c, quarter:].astype(jnp.float32)).astype(jnp.bfloat16)
        remote(sx.at[c], rx.at[c], x_send.at[c], x_recv.at[c], to_x)
        keep[c, :quarter] = keep[c, :quarter] + rt[c, :quarter].astype(jnp.float32)
    for c in range(chunks):
        landed(rx.at[c], x_send.at[c], x_recv.at[c])
        value = keep[c, :quarter] + rx[c].astype(jnp.float32)
        value = value.reshape(planes, rows, span)
        sz[c] = value.astype(jnp.bfloat16)
        for q in reversed(near):
            remote(sz.at[c, q], rz.at[c, p], z_send.at[c, q], z_recv.at[c, p], {"plane": q})
        vkeep[c] = value
    for c in range(chunks):
        value = vkeep[c, p]
        for q in near:
            landed(rz.at[c, q], z_send.at[c, q], z_recv.at[c, q])
            value = value + rz[c, q].astype(jnp.float32)
        out_ref[:, c * span : (c + 1) * span] = value.astype(jnp.bfloat16)
    for copy in pending:
        copy.wait_send()


def fused_block(planes, tokens, expert_ids, slot_index, route_weight, shared_gate, shared_gate_up, shared_down, expert_gate_up, expert_down):
    rows, width = tokens.shape
    units = shared_down.shape[0]
    panel = -(-(units // LANES) // 4) * LANES
    chunks = COLUMN_CHUNKS
    span = width // chunks
    bf16, f32 = jnp.bfloat16, jnp.float32
    anywhere = pl.BlockSpec(memory_space=pl.ANY)
    vmem = pl.BlockSpec(memory_space=pltpu.VMEM)
    blocks = 4 * planes
    return pl.pallas_call(
        functools.partial(block_kernel, planes),
        out_shape=jax.ShapeDtypeStruct((rows, width), bf16),
        in_specs=[anywhere] * 4 + [vmem] + [anywhere] * 4,
        out_specs=vmem,
        scratch_shapes=[
            pltpu.VMEM((blocks, rows, width + LANES), bf16),
            pltpu.VMEM(expert_ids.shape, jnp.int32),
            pltpu.VMEM(slot_index.shape, jnp.int32),
            pltpu.VMEM(route_weight.shape, bf16),
            pltpu.VMEM((2, width, panel), bf16),
            pltpu.VMEM((panel, width), bf16),
            pltpu.VMEM(expert_gate_up.shape[1:], bf16),
            pltpu.VMEM(expert_down.shape[1:], bf16),
            pltpu.VMEM((chunks, 2 * planes * rows, span), f32),
            pltpu.VMEM((chunks, 2 * planes * rows, span), bf16),
            pltpu.VMEM((chunks, 2 * planes * rows, span), bf16),
            pltpu.VMEM((chunks, planes * rows, span), bf16),
            pltpu.VMEM((chunks, planes * rows, span), bf16),
            pltpu.VMEM((chunks, planes, rows, span), f32),
            pltpu.VMEM((chunks, planes, rows, span), bf16),
            pltpu.VMEM((chunks, planes, rows, span), bf16),
            pltpu.SemaphoreType.DMA((8,)),
            pltpu.SemaphoreType.DMA((4, planes)),
            pltpu.SemaphoreType.DMA((4, planes)),
            pltpu.SemaphoreType.DMA((chunks,)),
            pltpu.SemaphoreType.DMA((chunks,)),
            pltpu.SemaphoreType.DMA((chunks,)),
            pltpu.SemaphoreType.DMA((chunks,)),
            pltpu.SemaphoreType.DMA((chunks, planes)),
            pltpu.SemaphoreType.DMA((chunks, planes)),
        ],
        compiler_params=pltpu.CompilerParams(collective_id=0, has_side_effects=True),
        name="expert_block",
    )(tokens, expert_ids, slot_index, route_weight, shared_gate.reshape(1, width), shared_gate_up, shared_down, expert_gate_up, expert_down)


def on_any_device(mesh, tokens, expert_ids, slot_index, route_weight, shared_gate, shared_gate_up, shared_down, expert_gate_up, expert_down):
    args = (tokens, expert_ids, slot_index, route_weight, shared_gate, shared_gate_up, shared_down, expert_gate_up, expert_down)
    planes = mesh.shape["plane"]
    every_expert = expert_ids.shape[1] == planes * expert_gate_up.shape[0] and expert_gate_up.shape[0] == 1
    pairs = mesh.shape["depth"] == 2 and mesh.shape["tok"] == 2
    tiled = tokens.shape[1] % (LANES * COLUMN_CHUNKS) == 0 and shared_down.shape[0] % LANES == 0
    if every_expert and pairs and tiled:
        return fused_block(planes, *args)
    return on_device(*args)


def solution(mesh):
    in_specs = (
        P(("groups", "plane", "depth", "tok"), None),
        P(("groups", "plane", "depth", "tok"), None),
        P(("groups", "plane", "depth", "tok"), None),
        P(("groups", "plane", "depth", "tok"), None),
        P(),
        P(None, None, "plane"),
        P("plane", None),
        P("plane", None, None, ("depth", "tok")),
        P("plane", ("depth", "tok"), None),
    )
    out_specs = P(("groups", "plane", "depth", "tok"), None)
    return jax.shard_map(
        functools.partial(on_any_device, mesh), mesh=mesh, in_specs=in_specs, out_specs=out_specs, check_vma=False
    )
```

```python
import functools

import jax
import jax.numpy as jnp
from jax import lax
from jax.experimental import pallas as pl
from jax.experimental.pallas import tpu as pltpu
from jax.sharding import PartitionSpec as P


def gated_rows(token_rows, gate_up):
    gate_part = jnp.dot(token_rows, gate_up[0], preferred_element_type=jnp.float32)
    up_part = jnp.dot(token_rows, gate_up[1], preferred_element_type=jnp.float32)
    return (jax.nn.silu(gate_part) * up_part).astype(jnp.bfloat16)


def expert_rows(received, gate_up, down_proj):
    hidden = gated_rows(lax.all_gather(received, ("depth", "tok"), axis=0, tiled=True), gate_up)
    return lax.psum_scatter(
        jnp.dot(hidden, down_proj, preferred_element_type=jnp.float32).astype(jnp.bfloat16),
        ("depth", "tok"),
        scatter_dimension=0,
        tiled=True,
    ).astype(jnp.float32)


def on_device(
    tokens,
    expert_ids,
    slot_index,
    route_weight,
    shared_gate,
    shared_gate_up,
    shared_down,
    expert_gate_up,
    expert_down,
):
    planes = lax.axis_size("plane")
    tok_rows = tokens.shape[0]
    choose_count = expert_ids.shape[1]
    model_width = tokens.shape[1]
    capacity = max(2, tok_rows * choose_count // planes)
    slot_total = planes * capacity
    local_gate_up = expert_gate_up[0]
    local_down = expert_down[0]
    column = lax.broadcasted_iota(jnp.int32, (slot_total, 1, 1), 0)
    kept_mask = slot_index < capacity
    target = jnp.where(kept_mask, expert_ids * capacity + slot_index, -1)
    matches = target[None, :, :] == column
    spread = jnp.any(matches, axis=2).astype(jnp.bfloat16)
    outgoing = jnp.dot(spread, tokens, preferred_element_type=jnp.float32).astype(jnp.bfloat16)
    outgoing = outgoing.reshape(planes, capacity, model_width)
    routed_slots = lax.all_to_all(
        expert_rows(
            lax.all_to_all(outgoing, "plane", split_axis=0, concat_axis=0, tiled=True),
            local_gate_up,
            local_down,
        ).astype(jnp.bfloat16),
        "plane",
        split_axis=0,
        concat_axis=0,
        tiled=True,
    ).astype(jnp.float32)
    weights = route_weight.astype(jnp.float32)
    combine = jnp.sum(jnp.where(matches, weights[None, :, :], 0.0), axis=2).T
    routed = jnp.dot(
        combine,
        routed_slots.reshape(slot_total, model_width),
        precision=lax.Precision.HIGHEST,
        preferred_element_type=jnp.float32,
    )
    shared_hidden = gated_rows(lax.all_gather(tokens, "plane", axis=0, tiled=True), shared_gate_up)
    shared_out = lax.psum_scatter(
        jnp.dot(shared_hidden, shared_down, preferred_element_type=jnp.float32).astype(
            jnp.bfloat16
        ),
        "plane",
        scatter_dimension=0,
        tiled=True,
    ).astype(jnp.float32)
    shared_scale = jax.nn.sigmoid(jnp.dot(tokens, shared_gate, preferred_element_type=jnp.float32))
    result = shared_scale[:, None] * shared_out + routed
    return result.astype(jnp.bfloat16)


LANES = 128
COLUMN_CHUNKS = 4
MESH = pl.DeviceIdType.MESH


def planes_by_distance(me, planes):
    orders = [sorted((q for q in range(planes) if q != p), key=lambda q: abs(q - p)) for p in range(planes)]
    picked = []
    for place in range(planes - 1):
        value = jnp.int32(orders[0][place])
        for p in range(1, planes):
            value = jnp.where(me == p, jnp.int32(orders[p][place]), value)
        picked.append(value)
    return picked


def by_rows(left, right):
    return lax.dot_general(left, right, (((1,), (1,)), ((), ())), preferred_element_type=jnp.float32)


def block_kernel(
    planes,
    tok_hbm,
    ids_hbm,
    slot_hbm,
    rw_hbm,
    sg_ref,
    sgu_hbm,
    sdn_hbm,
    egu_hbm,
    edn_hbm,
    out_ref,
    xb,
    ids_v,
    slot_v,
    rw_v,
    sgu_v,
    sdn_v,
    egu_v,
    edn_v,
    keep,
    st,
    rt,
    sx,
    rx,
    vkeep,
    sz,
    rz,
    local_sem,
    ag_send,
    ag_recv,
    t_send,
    t_recv,
    x_send,
    x_recv,
    z_send,
    z_recv,
):
    p = lax.axis_index("plane")
    d = lax.axis_index("depth")
    t = lax.axis_index("tok")
    rows, width = tok_hbm.shape
    choices = ids_hbm.shape[0]
    shared_units = sdn_hbm.shape[0]
    panel = sdn_v.shape[0]
    chunks = st.shape[0]
    span = width // chunks
    half = st.shape[1]
    quarter = half // 2
    near = planes_by_distance(p, planes)
    to_x = {"depth": 1 - d}
    to_t = {"tok": 1 - t}

    shard = d * 2 + t
    start = pl.multiple_of(jnp.minimum(shard * panel, shared_units - panel), LANES)

    def local(src, dst, index):
        copy = pltpu.make_async_copy(src, dst, local_sem.at[index])
        copy.start()
        return copy

    tok_copy = local(tok_hbm, xb.at[p, :, pl.ds(0, width)], 0)
    small = [
        local(ids_hbm, ids_v, 1),
        local(slot_hbm, slot_v, 2),
        local(rw_hbm, rw_v, 3),
    ]
    barrier = pltpu.get_barrier_semaphore()
    for peer in [{"plane": q} for q in near] + [to_x, to_t]:
        pl.semaphore_signal(barrier, inc=1, device_id=peer, device_id_type=MESH)
    up_copies = [
        local(egu_hbm.at[0], egu_v, 4),
        local(sgu_hbm.at[:, :, pl.ds(start, panel)], sgu_v, 5),
    ]
    down_copies = [
        local(edn_hbm.at[0], edn_v, 6),
        local(sdn_hbm.at[pl.ds(start, panel), :], sdn_v, 7),
    ]

    for copy in small:
        copy.wait()
    expert = lax.broadcasted_iota(jnp.int32, (LANES, rows), 0)
    ids = ids_v[...]
    slots = slot_v[...]
    weights = rw_v[...].astype(jnp.float32)
    capacity = max(2, rows * choices // planes)
    share = jnp.zeros((LANES, rows), jnp.float32)
    for k in range(choices):
        hit = (ids[k : k + 1] == expert) & (slots[k : k + 1] < capacity)
        share = share + jnp.where(hit, weights[k : k + 1], 0.0)
    same_row = lax.broadcasted_iota(jnp.int32, (rows, rows), 0) == lax.broadcasted_iota(jnp.int32, (rows, rows), 1)
    turned = by_rows(same_row.astype(jnp.bfloat16), share.astype(jnp.bfloat16))
    xb[p, :, width:] = turned.astype(jnp.bfloat16)
    tok_copy.wait()
    pl.semaphore_wait(barrier, planes + 1)

    def block(rel_t, rel_d, q):
        return xb.at[(rel_t * 2 + rel_d) * planes + q]

    pending = []

    def remote(src, dst, send_sem, recv_sem, device):
        copy = pltpu.make_async_remote_copy(
            src_ref=src,
            dst_ref=dst,
            send_sem=send_sem,
            recv_sem=recv_sem,
            device_id=device,
            device_id_type=MESH,
        )
        copy.start()
        pending.append(copy)

    def landed(dst, send_sem, recv_sem):
        pltpu.make_async_remote_copy(
            src_ref=dst,
            dst_ref=dst,
            send_sem=send_sem,
            recv_sem=recv_sem,
            device_id=to_t,
            device_id_type=MESH,
        ).wait_recv()

    for q in reversed(near):
        remote(block(0, 0, p), block(0, 0, p), ag_send.at[0, q], ag_recv.at[0, p], {"plane": q})

    def pass_x(q):
        remote(block(0, 0, q), block(0, 1, q), ag_send.at[1, q], ag_recv.at[1, q], to_x)

    def pass_t(rel_d, q):
        remote(block(0, rel_d, q), block(1, rel_d, q), ag_send.at[2 + rel_d, q], ag_recv.at[2 + rel_d, q], to_t)

    def from_z(q):
        landed(block(0, 0, q), ag_send.at[0, q], ag_recv.at[0, q])
        pass_x(q)
        pass_t(0, q)

    def from_x(q):
        landed(block(0, 1, q), ag_send.at[1, q], ag_recv.at[1, q])
        pass_t(1, q)

    pass_x(p)
    pass_t(0, p)
    from_z(near[0])
    from_x(p)
    for place in range(1, planes - 1):
        from_z(near[place])
        from_x(near[place - 1])
    from_x(near[-1])
    for copy in up_copies:
        copy.wait()
    for rel_d in range(2):
        for q in [p] + near:
            landed(block(1, rel_d, q), ag_send.at[2 + rel_d, q], ag_recv.at[2 + rel_d, q])

    total = xb.shape[0] * rows
    x = xb[:, :, :width].reshape(total, width)

    expert_hidden = (jax.nn.silu(by_rows(x, egu_v[0])) * by_rows(x, egu_v[1])).astype(jnp.bfloat16)
    gate_part = jnp.dot(x, sgu_v[0], preferred_element_type=jnp.float32)
    up_part = jnp.dot(x, sgu_v[1], preferred_element_type=jnp.float32)
    shared_hidden = jax.nn.silu(gate_part) * up_part
    unit = start + lax.broadcasted_iota(jnp.int32, shared_hidden.shape, 1)
    shared_hidden = jnp.where(unit >= shard * panel, shared_hidden, 0.0).astype(jnp.bfloat16)
    column = lax.broadcasted_iota(jnp.int32, (total, LANES), 1)
    meta = xb[:, :, width:].reshape(total, LANES).astype(jnp.float32)
    route = jnp.sum(jnp.where(column == p, meta, 0.0), axis=1, keepdims=True)
    gate_rows = jnp.broadcast_to(sg_ref[...].reshape(1, width), (8, width))
    score = by_rows(x, gate_rows)
    scale = jax.nn.sigmoid(score[:, :1])

    for copy in down_copies:
        copy.wait()
    for c in range(chunks):
        cols = pl.ds(c * span, span)
        part = route * jnp.dot(expert_hidden, edn_v[:, cols], preferred_element_type=jnp.float32)
        part = part + scale * jnp.dot(shared_hidden, sdn_v[:, cols], preferred_element_type=jnp.float32)
        st[c] = part[half:].astype(jnp.bfloat16)
        remote(st.at[c], rt.at[c], t_send.at[c], t_recv.at[c], to_t)
        keep[c] = part[:half]
    for c in range(chunks):
        landed(rt.at[c], t_send.at[c], t_recv.at[c])
        sx[c] = (keep[c, quarter:] + rt[c, quarter:].astype(jnp.float32)).astype(jnp.bfloat16)
        remote(sx.at[c], rx.at[c], x_send.at[c], x_recv.at[c], to_x)
        keep[c, :quarter] = keep[c, :quarter] + rt[c, :quarter].astype(jnp.float32)
    for c in range(chunks):
        landed(rx.at[c], x_send.at[c], x_recv.at[c])
        value = keep[c, :quarter] + rx[c].astype(jnp.float32)
        value = value.reshape(planes, rows, span)
        sz[c] = value.astype(jnp.bfloat16)
        for q in reversed(near):
            remote(sz.at[c, q], rz.at[c, p], z_send.at[c, q], z_recv.at[c, p], {"plane": q})
        vkeep[c] = value
    for c in range(chunks):
        value = vkeep[c, p]
        for q in near:
            landed(rz.at[c, q], z_send.at[c, q], z_recv.at[c, q])
            value = value + rz[c, q].astype(jnp.float32)
        out_ref[:, c * span : (c + 1) * span] = value.astype(jnp.bfloat16)
    for copy in pending:
        copy.wait_send()


def fused_block(planes, tokens, expert_ids, slot_index, route_weight, shared_gate, shared_gate_up, shared_down, expert_gate_up, expert_down):
    rows, width = tokens.shape
    units = shared_down.shape[0]
    panel = -(-(units // LANES) // 4) * LANES
    chunks = COLUMN_CHUNKS
    span = width // chunks
    bf16, f32 = jnp.bfloat16, jnp.float32
    anywhere = pl.BlockSpec(memory_space=pl.ANY)
    vmem = pl.BlockSpec(memory_space=pltpu.VMEM)
    blocks = 4 * planes
    return pl.pallas_call(
        functools.partial(block_kernel, planes),
        out_shape=jax.ShapeDtypeStruct((rows, width), bf16),
        in_specs=[anywhere] * 4 + [vmem] + [anywhere] * 4,
        out_specs=vmem,
        scratch_shapes=[
            pltpu.VMEM((blocks, rows, width + LANES), bf16),
            pltpu.VMEM(expert_ids.shape[::-1], jnp.int32),
            pltpu.VMEM(slot_index.shape[::-1], jnp.int32),
            pltpu.VMEM(route_weight.shape[::-1], bf16),
            pltpu.VMEM((2, width, panel), bf16),
            pltpu.VMEM((panel, width), bf16),
            pltpu.VMEM((2, expert_gate_up.shape[3], width), bf16),
            pltpu.VMEM(expert_down.shape[1:], bf16),
            pltpu.VMEM((chunks, 2 * planes * rows, span), f32),
            pltpu.VMEM((chunks, 2 * planes * rows, span), bf16),
            pltpu.VMEM((chunks, 2 * planes * rows, span), bf16),
            pltpu.VMEM((chunks, planes * rows, span), bf16),
            pltpu.VMEM((chunks, planes * rows, span), bf16),
            pltpu.VMEM((chunks, planes, rows, span), f32),
            pltpu.VMEM((chunks, planes, rows, span), bf16),
            pltpu.VMEM((chunks, planes, rows, span), bf16),
            pltpu.SemaphoreType.DMA((8,)),
            pltpu.SemaphoreType.DMA((4, planes)),
            pltpu.SemaphoreType.DMA((4, planes)),
            pltpu.SemaphoreType.DMA((chunks,)),
            pltpu.SemaphoreType.DMA((chunks,)),
            pltpu.SemaphoreType.DMA((chunks,)),
            pltpu.SemaphoreType.DMA((chunks,)),
            pltpu.SemaphoreType.DMA((chunks, planes)),
            pltpu.SemaphoreType.DMA((chunks, planes)),
        ],
        compiler_params=pltpu.CompilerParams(collective_id=0, has_side_effects=True),
        name="expert_block",
    )(tokens, expert_ids.T, slot_index.T, route_weight.T, shared_gate, shared_gate_up, shared_down, jnp.swapaxes(expert_gate_up, 2, 3), expert_down)


def on_any_device(mesh, tokens, expert_ids, slot_index, route_weight, shared_gate, shared_gate_up, shared_down, expert_gate_up, expert_down):
    args = (tokens, expert_ids, slot_index, route_weight, shared_gate, shared_gate_up, shared_down, expert_gate_up, expert_down)
    planes = mesh.shape["plane"]
    every_expert = expert_ids.shape[1] == planes * expert_gate_up.shape[0] and expert_gate_up.shape[0] == 1
    pairs = mesh.shape["depth"] == 2 and mesh.shape["tok"] == 2
    tiled = tokens.shape[1] % (LANES * COLUMN_CHUNKS) == 0 and shared_down.shape[0] % LANES == 0
    if every_expert and pairs and tiled:
        return fused_block(planes, *args)
    return on_device(*args)


def solution(mesh):
    in_specs = (
        P(("groups", "plane", "depth", "tok"), None),
        P(("groups", "plane", "depth", "tok"), None),
        P(("groups", "plane", "depth", "tok"), None),
        P(("groups", "plane", "depth", "tok"), None),
        P(),
        P(None, None, "plane"),
        P("plane", None),
        P("plane", None, None, ("depth", "tok")),
        P("plane", ("depth", "tok"), None),
    )
    out_specs = P(("groups", "plane", "depth", "tok"), None)
    return jax.shard_map(
        functools.partial(on_any_device, mesh), mesh=mesh, in_specs=in_specs, out_specs=out_specs, check_vma=False
    )
```

```python
import functools

import jax
import jax.numpy as jnp
from jax import lax
from jax.experimental import pallas as pl
from jax.experimental.pallas import tpu as pltpu
from jax.sharding import PartitionSpec as P


def gated_rows(token_rows, gate_up):
    gate_part = jnp.dot(token_rows, gate_up[0], preferred_element_type=jnp.float32)
    up_part = jnp.dot(token_rows, gate_up[1], preferred_element_type=jnp.float32)
    return (jax.nn.silu(gate_part) * up_part).astype(jnp.bfloat16)


def expert_rows(received, gate_up, down_proj):
    hidden = gated_rows(lax.all_gather(received, ("depth", "tok"), axis=0, tiled=True), gate_up)
    return lax.psum_scatter(
        jnp.dot(hidden, down_proj, preferred_element_type=jnp.float32).astype(jnp.bfloat16),
        ("depth", "tok"),
        scatter_dimension=0,
        tiled=True,
    ).astype(jnp.float32)


def on_device(
    tokens,
    expert_ids,
    slot_index,
    route_weight,
    shared_gate,
    shared_gate_up,
    shared_down,
    expert_gate_up,
    expert_down,
):
    planes = lax.axis_size("plane")
    tok_rows = tokens.shape[0]
    choose_count = expert_ids.shape[1]
    model_width = tokens.shape[1]
    capacity = max(2, tok_rows * choose_count // planes)
    slot_total = planes * capacity
    local_gate_up = expert_gate_up[0]
    local_down = expert_down[0]
    column = lax.broadcasted_iota(jnp.int32, (slot_total, 1, 1), 0)
    kept_mask = slot_index < capacity
    target = jnp.where(kept_mask, expert_ids * capacity + slot_index, -1)
    matches = target[None, :, :] == column
    spread = jnp.any(matches, axis=2).astype(jnp.bfloat16)
    outgoing = jnp.dot(spread, tokens, preferred_element_type=jnp.float32).astype(jnp.bfloat16)
    outgoing = outgoing.reshape(planes, capacity, model_width)
    routed_slots = lax.all_to_all(
        expert_rows(
            lax.all_to_all(outgoing, "plane", split_axis=0, concat_axis=0, tiled=True),
            local_gate_up,
            local_down,
        ).astype(jnp.bfloat16),
        "plane",
        split_axis=0,
        concat_axis=0,
        tiled=True,
    ).astype(jnp.float32)
    weights = route_weight.astype(jnp.float32)
    combine = jnp.sum(jnp.where(matches, weights[None, :, :], 0.0), axis=2).T
    routed = jnp.dot(
        combine,
        routed_slots.reshape(slot_total, model_width),
        precision=lax.Precision.HIGHEST,
        preferred_element_type=jnp.float32,
    )
    shared_hidden = gated_rows(lax.all_gather(tokens, "plane", axis=0, tiled=True), shared_gate_up)
    shared_out = lax.psum_scatter(
        jnp.dot(shared_hidden, shared_down, preferred_element_type=jnp.float32).astype(
            jnp.bfloat16
        ),
        "plane",
        scatter_dimension=0,
        tiled=True,
    ).astype(jnp.float32)
    shared_scale = jax.nn.sigmoid(jnp.dot(tokens, shared_gate, preferred_element_type=jnp.float32))
    result = shared_scale[:, None] * shared_out + routed
    return result.astype(jnp.bfloat16)


LANES = 128
COLUMN_CHUNKS = 8
T_LAG = 3
REACH = 2
MESH = pl.DeviceIdType.MESH


def planes_by_distance(me, planes):
    orders = [sorted((q for q in range(planes) if q != p), key=lambda q: abs(q - p)) for p in range(planes)]
    picked = []
    for place in range(planes - 1):
        value = jnp.int32(orders[0][place])
        for p in range(1, planes):
            value = jnp.where(me == p, jnp.int32(orders[p][place]), value)
        picked.append(value)
    return picked


def by_rows(left, right):
    return lax.dot_general(left, right, (((1,), (1,)), ((), ())), preferred_element_type=jnp.float32)


def block_kernel(
    planes,
    tok_hbm,
    ids_hbm,
    slot_hbm,
    rw_hbm,
    sg_ref,
    sgu_hbm,
    sdn_hbm,
    egu_hbm,
    edn_hbm,
    out_ref,
    xb,
    ids_v,
    slot_v,
    rw_v,
    sgu_v,
    sdn_v,
    egu_v,
    edn_v,
    keep,
    st,
    rt,
    sx,
    rx,
    vkeep,
    sz,
    rz,
    local_sem,
    ag_send,
    ag_recv,
    t_send,
    t_recv,
    x_send,
    x_recv,
    z_send,
    z_recv,
):
    p = lax.axis_index("plane")
    d = lax.axis_index("depth")
    t = lax.axis_index("tok")
    rows, width = tok_hbm.shape
    choices = ids_hbm.shape[0]
    shared_units = sdn_hbm.shape[0]
    panel = sdn_v.shape[0]
    chunks = st.shape[0]
    span = width // chunks
    half = st.shape[1]
    quarter = half // 2
    near = planes_by_distance(p, planes)
    to_x = {"depth": 1 - d}
    to_t = {"tok": 1 - t}

    shard = d * 2 + t
    start = pl.multiple_of(jnp.minimum(shard * panel, shared_units - panel), LANES)

    def local(src, dst, index):
        copy = pltpu.make_async_copy(src, dst, local_sem.at[index])
        copy.start()
        return copy

    tok_copy = local(tok_hbm, xb.at[p, :, pl.ds(0, width)], 0)
    small = [
        local(ids_hbm, ids_v, 1),
        local(slot_hbm, slot_v, 2),
        local(rw_hbm, rw_v, 3),
    ]
    inner = (p > 0) & (p < planes - 1)
    barrier = pltpu.get_barrier_semaphore()
    for peer in [{"plane": q} for q in near[:-1]] + [to_x, to_t]:
        pl.semaphore_signal(barrier, inc=1, device_id=peer, device_id_type=MESH)

    @pl.when(inner)
    def _():
        pl.semaphore_signal(barrier, inc=1, device_id={"plane": near[-1]}, device_id_type=MESH)

    up_copies = [
        local(egu_hbm.at[0], egu_v, 4),
        local(sgu_hbm.at[0, :, pl.ds(start, panel)], sgu_v.at[:, pl.ds(0, panel)], 5),
        local(sgu_hbm.at[1, :, pl.ds(start, panel)], sgu_v.at[:, pl.ds(panel, panel)], 8),
    ]
    down_copies = [
        local(edn_hbm.at[0], edn_v, 6),
        local(sdn_hbm.at[pl.ds(start, panel), :], sdn_v, 7),
    ]

    for copy in small:
        copy.wait()
    expert = lax.broadcasted_iota(jnp.int32, (LANES, rows), 0)
    ids = ids_v[...]
    slots = slot_v[...]
    weights = rw_v[...].astype(jnp.float32)
    capacity = max(2, rows * choices // planes)
    share = jnp.zeros((LANES, rows), jnp.float32)
    for k in range(choices):
        hit = (ids[k : k + 1] == expert) & (slots[k : k + 1] < capacity)
        share = share + jnp.where(hit, weights[k : k + 1], 0.0)
    same_row = lax.broadcasted_iota(jnp.int32, (rows, rows), 0) == lax.broadcasted_iota(jnp.int32, (rows, rows), 1)
    turned = by_rows(same_row.astype(jnp.bfloat16), share.astype(jnp.bfloat16))
    xb[p, :, width:] = turned.astype(jnp.bfloat16)
    tok_copy.wait()
    pl.semaphore_wait(barrier, jnp.where(inner, planes + 1, planes))

    def block(rel_t, rel_d, q):
        return xb.at[(rel_t * 2 + rel_d) * planes + q]

    pending = []

    def copy_to(src, dst, send_sem, recv_sem, device):
        return pltpu.make_async_remote_copy(
            src_ref=src,
            dst_ref=dst,
            send_sem=send_sem,
            recv_sem=recv_sem,
            device_id=device,
            device_id_type=MESH,
        )

    def remote(*what):
        copy = copy_to(*what)
        copy.start()
        pending.append(copy)

    def landed(dst, send_sem, recv_sem):
        pltpu.make_async_remote_copy(
            src_ref=dst,
            dst_ref=dst,
            send_sem=send_sem,
            recv_sem=recv_sem,
            device_id=to_t,
            device_id_type=MESH,
        ).wait_recv()

    def own_to(q):
        return copy_to(block(0, 0, p), block(0, 0, p), ag_send.at[0, q], ag_recv.at[0, p], {"plane": q})

    beside = jnp.where(p == 1, 0, planes - 1)
    relay = copy_to(block(0, 0, near[-1]), block(0, 0, near[-1]), ag_send.at[4, 0], ag_recv.at[0, near[-1]], {"plane": beside})

    @pl.when(inner)
    def _():
        own_to(near[-1]).start()

    for q in reversed(near[:-1]):
        copy = own_to(q)
        copy.start()
        pending.append(copy)

    def pass_x(q):
        remote(block(0, 0, q), block(0, 1, q), ag_send.at[1, q], ag_recv.at[1, q], to_x)

    def pass_t(rel_d, q):
        remote(block(0, rel_d, q), block(1, rel_d, q), ag_send.at[2 + rel_d, q], ag_recv.at[2 + rel_d, q], to_t)

    def from_z(q):
        landed(block(0, 0, q), ag_send.at[0, q], ag_recv.at[0, q])
        if q is near[-1]:
            pl.when(inner)(relay.start)
        pass_x(q)
        pass_t(0, q)

    def from_x(q):
        landed(block(0, 1, q), ag_send.at[1, q], ag_recv.at[1, q])
        pass_t(1, q)

    pass_x(p)
    pass_t(0, p)
    from_z(near[0])
    from_x(p)
    for place in range(1, planes - 1):
        from_z(near[place])
        from_x(near[place - 1])
    from_x(near[-1])
    for copy in up_copies:
        copy.wait()
    for rel_d in range(2):
        for q in [p] + near:
            landed(block(1, rel_d, q), ag_send.at[2 + rel_d, q], ag_recv.at[2 + rel_d, q])

    total = xb.shape[0] * rows
    x = xb[:, :, :width].reshape(total, width)

    expert_hidden = (jax.nn.silu(by_rows(x, egu_v[0])) * by_rows(x, egu_v[1])).astype(jnp.bfloat16)
    both_parts = jnp.dot(x, sgu_v[...], preferred_element_type=jnp.float32)
    shared_hidden = jax.nn.silu(both_parts[:, :panel]) * both_parts[:, panel:]
    unit = start + lax.broadcasted_iota(jnp.int32, shared_hidden.shape, 1)
    shared_hidden = jnp.where(unit >= shard * panel, shared_hidden, 0.0).astype(jnp.bfloat16)
    column = lax.broadcasted_iota(jnp.int32, (total, LANES), 1)
    meta = xb[:, :, width:].reshape(total, LANES).astype(jnp.float32)
    route = jnp.sum(jnp.where(column == p, meta, 0.0), axis=1, keepdims=True)
    gate_rows = jnp.broadcast_to(sg_ref[...].reshape(1, width), (8, width))
    score = by_rows(x, gate_rows)
    scale = jax.nn.sigmoid(score[:, :1])

    for copy in down_copies:
        copy.wait()

    def down(c):
        cols = pl.ds(c * span, span)
        part = route * jnp.dot(expert_hidden, edn_v[:, cols], preferred_element_type=jnp.float32)
        part = part + scale * jnp.dot(shared_hidden, sdn_v[:, cols], preferred_element_type=jnp.float32)
        st[c] = part[half:].astype(jnp.bfloat16)
        remote(st.at[c], rt.at[c], t_send.at[c], t_recv.at[c], to_t)
        keep[c] = part[:half]

    def after_t(c):
        landed(rt.at[c], t_send.at[c], t_recv.at[c])
        sx[c] = (keep[c, quarter:] + rt[c, quarter:].astype(jnp.float32)).astype(jnp.bfloat16)
        remote(sx.at[c], rx.at[c], x_send.at[c], x_recv.at[c], to_x)
        keep[c, :quarter] = keep[c, :quarter] + rt[c, :quarter].astype(jnp.float32)

    for c in range(chunks):
        down(c)
        if c >= T_LAG:
            after_t(c - T_LAG)
    for c in range(chunks - T_LAG, chunks):
        after_t(c)
    for c in range(chunks):
        landed(rx.at[c], x_send.at[c], x_recv.at[c])
        value = keep[c, :quarter] + rx[c].astype(jnp.float32)
        value = value.reshape(planes, rows, span)
        sz[c] = value.astype(jnp.bfloat16)
        for q in reversed(near):
            remote(sz.at[c, q], rz.at[c, p], z_send.at[c, q], z_recv.at[c, p], {"plane": q})
        vkeep[c] = value
    for c in range(chunks):
        value = vkeep[c, p]
        for q in near:
            landed(rz.at[c, q], z_send.at[c, q], z_recv.at[c, q])
            value = value + rz[c, q].astype(jnp.float32)
        out_ref[:, c * span : (c + 1) * span] = value.astype(jnp.bfloat16)
    for copy in pending:
        copy.wait_send()

    @pl.when(inner)
    def _():
        own_to(near[-1]).wait_send()
        relay.wait_send()


def fused_block(planes, tokens, expert_ids, slot_index, route_weight, shared_gate, shared_gate_up, shared_down, expert_gate_up, expert_down):
    rows, width = tokens.shape
    units = shared_down.shape[0]
    panel = -(-(units // LANES) // 4) * LANES
    chunks = COLUMN_CHUNKS
    span = width // chunks
    bf16, f32 = jnp.bfloat16, jnp.float32
    anywhere = pl.BlockSpec(memory_space=pl.ANY)
    vmem = pl.BlockSpec(memory_space=pltpu.VMEM)
    blocks = 4 * planes
    return pl.pallas_call(
        functools.partial(block_kernel, planes),
        out_shape=jax.ShapeDtypeStruct((rows, width), bf16),
        in_specs=[anywhere] * 4 + [vmem] + [anywhere] * 4,
        out_specs=vmem,
        scratch_shapes=[
            pltpu.VMEM((blocks, rows, width + LANES), bf16),
            pltpu.VMEM(expert_ids.shape[::-1], jnp.int32),
            pltpu.VMEM(slot_index.shape[::-1], jnp.int32),
            pltpu.VMEM(route_weight.shape[::-1], bf16),
            pltpu.VMEM((width, 2 * panel), bf16),
            pltpu.VMEM((panel, width), bf16),
            pltpu.VMEM((2, expert_gate_up.shape[3], width), bf16),
            pltpu.VMEM(expert_down.shape[1:], bf16),
            pltpu.VMEM((chunks, 2 * planes * rows, span), f32),
            pltpu.VMEM((chunks, 2 * planes * rows, span), bf16),
            pltpu.VMEM((chunks, 2 * planes * rows, span), bf16),
            pltpu.VMEM((chunks, planes * rows, span), bf16),
            pltpu.VMEM((chunks, planes * rows, span), bf16),
            pltpu.VMEM((chunks, planes, rows, span), f32),
            pltpu.VMEM((chunks, planes, rows, span), bf16),
            pltpu.VMEM((chunks, planes, rows, span), bf16),
            pltpu.SemaphoreType.DMA((9,)),
            pltpu.SemaphoreType.DMA((5, planes)),
            pltpu.SemaphoreType.DMA((4, planes)),
            pltpu.SemaphoreType.DMA((chunks,)),
            pltpu.SemaphoreType.DMA((chunks,)),
            pltpu.SemaphoreType.DMA((chunks,)),
            pltpu.SemaphoreType.DMA((chunks,)),
            pltpu.SemaphoreType.DMA((chunks, planes)),
            pltpu.SemaphoreType.DMA((chunks, planes)),
        ],
        compiler_params=pltpu.CompilerParams(collective_id=0, has_side_effects=True),
        name="expert_block",
    )(tokens, expert_ids.T, slot_index.T, route_weight.T, shared_gate, shared_gate_up, shared_down, jnp.swapaxes(expert_gate_up, 2, 3), expert_down)


def on_any_device(mesh, tokens, expert_ids, slot_index, route_weight, shared_gate, shared_gate_up, shared_down, expert_gate_up, expert_down):
    args = (tokens, expert_ids, slot_index, route_weight, shared_gate, shared_gate_up, shared_down, expert_gate_up, expert_down)
    planes = mesh.shape["plane"]
    every_expert = expert_ids.shape[1] == planes * expert_gate_up.shape[0] and expert_gate_up.shape[0] == 1
    lined = planes == REACH + 2
    pairs = lined and mesh.shape["depth"] == 2 and mesh.shape["tok"] == 2
    tiled = tokens.shape[1] % (LANES * COLUMN_CHUNKS) == 0 and shared_down.shape[0] % LANES == 0
    if every_expert and pairs and tiled:
        return fused_block(planes, *args)
    return on_device(*args)


def solution(mesh):
    in_specs = (
        P(("groups", "plane", "depth", "tok"), None),
        P(("groups", "plane", "depth", "tok"), None),
        P(("groups", "plane", "depth", "tok"), None),
        P(("groups", "plane", "depth", "tok"), None),
        P(),
        P(None, None, "plane"),
        P("plane", None),
        P("plane", None, None, ("depth", "tok")),
        P("plane", ("depth", "tok"), None),
    )
    out_specs = P(("groups", "plane", "depth", "tok"), None)
    return jax.shard_map(
        functools.partial(on_any_device, mesh), mesh=mesh, in_specs=in_specs, out_specs=out_specs, check_vma=False
    )
```
